32 devices in a mesh: grp: 4 (over z), slab: 8 (over y, x, core).
Axes of the slice: x: 2, y: 2, z: 4, core: 2. Of those that a mesh axis runs over, the one named last changes fastest.
Arguments:
- orbitals: float32 [8, 96, 9216], P('grp', 'slab'), may hold values from -6 to 6
- occupation: int32 [8], P('grp'), may hold values from 1 to 4
- kernel_hat: float32 [192, 36864], P('slab'), may hold values from 0.02 to 1200, as said below
- pair_mask: int32 [1], replicated, may hold values from 1 to 3
Outputs:
- exchange_terms: float32 [8, 96, 9216], P('grp', 'slab')
The draws below stay inside these ranges and needn't reach their ends.
Inputs may be any that keep to these rules, and one draw needn't show every extreme that they name: In this round group g is paired with group g XOR pair_mask. kernel_hat is positive, and unchanged when each frequency index k is replaced by (192 - k) mod 192 in all three dimensions at once.
All inputs are finite; a program needn't handle non-finite values.
Results may differ from the reference program's by a relative error of at most 0.0001.
Values sent between devices are 32-bit elements; how exact they have to be, the bound alone decides.
A program may use at most 64 MiB of HBM per device.

```python
import math
import jax
import jax.numpy as jnp
from jax import lax

G = 96
P_SIZE = 192
ORBS = 2
ORBITALS = 8
N_GRP = 4


screening = 0.0025


def draw_kernel_hat(key, part):
    factors = jax.random.uniform(key, (P_SIZE, P_SIZE, P_SIZE), jnp.float32, 0.5, 1.5)
    mirrored = jnp.roll(jnp.flip(factors, (0, 1, 2)), 1, (0, 1, 2))
    even_factors = 0.5 * (factors + mirrored)
    wave_index = jnp.arange(P_SIZE, dtype=jnp.int32)
    folded = jnp.minimum(wave_index, P_SIZE - wave_index).astype(jnp.float32)
    eigen_line = 4.0 * jnp.sin(math.pi * folded / P_SIZE) ** 2
    eigen_sum = eigen_line[:, None, None] + eigen_line[None, :, None] + eigen_line[None, None, :]
    return (even_factors / (eigen_sum + screening)).reshape(P_SIZE, P_SIZE * P_SIZE)


def plant(entries, own_key, smallest, largest):
    spot = [jax.random.randint(jax.random.fold_in(own_key, axis), (), 0, length) for axis, length in enumerate(entries.shape)]
    main_axis = entries.shape.index(max(entries.shape))
    neighbour = spot[:main_axis] + [(spot[main_axis] + 1) % entries.shape[main_axis]] + spot[main_axis + 1:]
    return entries.at[tuple(spot)].set(smallest).at[tuple(neighbour)].set(largest)


def shard_levels(rng, dims, split, least, top_value):
    def one(position, blocks):
        steps = jax.random.uniform(jax.random.fold_in(jax.random.fold_in(rng, 6), position), (blocks,), jnp.float32, least / len(split), top_value / len(split))
        return jnp.repeat(jnp.exp(steps), dims[position] // blocks).reshape((-1,) + (1,) * (len(dims) - position - 1))

    loudness = one(*split[0])
    for cut in split[1:]:
        loudness = loudness * one(*cut)
    return loudness


def scatter_about(rng, dims, scale, reach, cuts=(), kind=jnp.bfloat16):
    level = shard_levels(rng, dims, cuts, -0.22, 0.18) if cuts else 1.0
    array = jax.random.normal(rng, dims, jnp.float32) * scale * level
    return jnp.minimum(jnp.maximum(array, -reach), reach).astype(kind)


def setup_inputs(seed: int = 0) -> dict:
    key_of = jax.random.split(jax.random.key(seed), 5)
    return {
        "orbitals": scatter_about(key_of[0], (ORBITALS, G, G * G), 1.0, 6.0, ((0, 4), (1, 8)), jnp.float32),
        "occupation": plant(jax.random.randint(key_of[1], (ORBITALS,), 1, 5), jax.random.fold_in(key_of[1], 1), 1, 4).astype(jnp.int32),
        "kernel_hat": draw_kernel_hat(jax.random.fold_in(key_of[4], 71), 0),
        "pair_mask": jax.random.randint(key_of[3], (1,), 1, N_GRP).astype(jnp.int32),
    }


def pair_potential(density, kernel_half):
    padded = jnp.pad(density, ((0, G), (0, G), (0, G)))
    spectrum = jnp.fft.rfftn(padded)
    field = jnp.fft.irfftn(spectrum * kernel_half, s=(P_SIZE, P_SIZE, P_SIZE))
    return field[:G, :G, :G]


def reference(orbitals, occupation, kernel_hat, pair_mask):
    fields = orbitals.reshape(N_GRP, ORBS, G, G, G)
    weights = (0.25 * occupation.astype(jnp.float32)).reshape(N_GRP, ORBS)
    kernel_cube = kernel_hat.reshape(P_SIZE, P_SIZE, P_SIZE)
    kernel_half = jnp.transpose(kernel_cube, (2, 1, 0))[:, :, : P_SIZE // 2 + 1]
    pair_bits = pair_mask[0].astype(jnp.int32)
    high_bit = jnp.zeros((), jnp.int32)
    for shift_level in range(1, 31):
        high_bit = high_bit + (jnp.right_shift(pair_bits, shift_level) > 0).astype(jnp.int32)
    low_bits = jnp.left_shift(jnp.ones((), jnp.int32), high_bit) - 1

    def pair_step(flat_index, sums):
        flat_index = flat_index.astype(jnp.int32)
        pair_index = flat_index // (ORBS * ORBS)
        first = (flat_index // ORBS) % ORBS
        second = flat_index % ORBS
        lower_group = jnp.bitwise_or(
            jnp.left_shift(jnp.right_shift(pair_index, high_bit), high_bit + 1),
            jnp.bitwise_and(pair_index, low_bits))
        upper_group = jnp.bitwise_xor(lower_group, pair_bits)
        left_field = fields[lower_group, first]
        right_field = fields[upper_group, second]
        potential = pair_potential(left_field * right_field, kernel_half)
        sums = sums.at[lower_group, first].add(-weights[upper_group, second] * potential * right_field)
        sums = sums.at[upper_group, second].add(-weights[lower_group, first] * potential * left_field)
        return sums

    total_pairs = (N_GRP // 2) * ORBS * ORBS
    sums = lax.fori_loop(0, total_pairs, pair_step, jnp.zeros((N_GRP, ORBS, G, G, G), jnp.float32))
    return sums.reshape(N_GRP * ORBS, G, G * G)
```

```python
import math

import jax
import jax.numpy as jnp
import ml_dtypes
import numpy as np
from jax import lax
from jax.experimental import pallas as pl
from jax.experimental.pallas import tpu as pltpu
from jax.sharding import PartitionSpec as P

LANE = 128


def halves(table):
    high = table.astype(np.float32).astype(ml_dtypes.bfloat16)
    low = (table - high.astype(np.float64)).astype(ml_dtypes.bfloat16)
    return np.stack([high, low])


class Plan:
    def __init__(self, planes, plane_cells, slabs, freqs):
        self.planes = planes
        self.grid = math.isqrt(plane_cells)
        self.slabs = slabs
        self.freqs = freqs
        self.period = 2 * self.grid
        self.group = math.lcm(self.grid, LANE)
        self.fold = self.group // self.grid
        self.chunks = self.grid // self.fold
        self.rows = planes * self.chunks
        self.groups = -(-planes // self.fold)
        self.lanes = self.groups * self.group
        self.wide = 2 * LANE
        self.starts = []
        for fold in range(self.fold):
            start = fold * self.grid // LANE * LANE
            self.starts.append(min(start, self.group - self.wide))
        self.spectrum = 2 * self.period
        self.padded = -(-self.period // self.wide) * self.wide

    def wave(self, left, right):
        angle = 2.0 * math.pi / self.period * (np.outer(left, right) % self.period)
        return np.cos(angle), np.sin(angle)

    def tables(self):
        grid, period, fold = self.grid, self.period, self.fold
        cells = np.arange(grid)
        waves = np.arange(period)
        cos, sin = self.wave(cells, waves)
        cosi, sini = cos.T / period, sin.T / period
        column = [
            (part, owner * self.freqs + own)
            for owner in range(self.slabs)
            for part in range(2)
            for own in range(self.freqs)
        ]
        part = np.array([c[0] for c in column])
        freq = np.array([c[1] for c in column])
        zf = np.zeros((fold, 2, self.wide, self.spectrum))
        zi = np.zeros((fold, self.spectrum, 2, self.wide))
        yf = np.zeros((fold, self.wide, 2, self.padded))
        yi = np.zeros((fold, self.padded, 2, self.wide))
        y_order = np.array([fold * q + j for j in range(fold) for q in range(self.chunks)])
        for j in range(fold):
            at = slice(j * grid - self.starts[j], (j + 1) * grid - self.starts[j])
            zf[j, 0, at] = np.where(part == 0, cos[:, freq], -sin[:, freq])
            zf[j, 1, at] = np.where(part == 0, sin[:, freq], cos[:, freq])
            zi[j, :, 0, at] = np.where(part == 0, cosi[freq].T, -sini[freq].T).T
            zi[j, :, 1, at] = np.where(part == 0, sini[freq].T, cosi[freq].T).T
            yf[j, at, 0, :period] = cos[y_order]
            yf[j, at, 1, :period] = sin[y_order]
            yi[j, :period, 0, at] = cosi[:, y_order]
            yi[j, :period, 1, at] = sini[:, y_order]
        row = [
            (c, s * self.planes + x)
            for x in range(self.planes)
            for s in range(self.slabs)
            for c in range(2)
        ]
        side = np.array([r[0] for r in row])
        cell = np.array([r[1] for r in row])
        xf = np.concatenate(
            [
                np.where(side == 0, cos[cell].T, sin[cell].T),
                np.where(side == 0, -sin[cell].T, cos[cell].T),
            ]
        )
        xi = np.concatenate(
            [
                np.where(side == 0, cosi[:, cell], sini[:, cell]),
                np.where(side == 0, -sini[:, cell], cosi[:, cell]),
            ]
        ).T
        return {
            "zf": halves(zf),
            "zi": halves(zi.reshape(fold, self.spectrum, 2 * self.wide)),
            "yf": halves(yf.reshape(fold, self.wide, 2 * self.padded)),
            "yi": halves(yi.reshape(fold, self.padded, 2 * self.wide)),
            "xf": halves(xf),
            "xi": halves(xi),
        }


def mm(left, right):
    return jnp.dot(left, right, preferred_element_type=jnp.float32)


def split(value):
    high = value.astype(jnp.bfloat16)
    low = (value - high.astype(jnp.float32)).astype(jnp.bfloat16)
    return high, low


def right_mul(value, high, low):
    vh, vl = value
    return mm(vh, high) + mm(vh, low) + mm(vl, high)


def left_mul(high, low, value):
    vh, vl = value
    return mm(high, vh) + mm(low, vh) + mm(high, vl)


def forward_z(plan, left_ref, right_ref, table_ref, out_ref, turned):
    right = right_ref[...]
    densities = [split(left_ref[i] * right) for i in range(2)]
    used = plan.planes * plan.grid
    if used < plan.lanes:
        turned[used:, :] = jnp.zeros((plan.lanes - used, plan.spectrum), jnp.float32)
    chunks, grid, wide = plan.chunks, plan.grid, plan.wide
    for j in range(plan.fold):
        at = slice(plan.starts[j], plan.starts[j] + wide)
        total = None
        for i in range(2):
            piece = tuple(d[:, at] for d in densities[i])
            term = right_mul(piece, table_ref[0, j, i], table_ref[1, j, i])
            total = term if total is None else total + term
        for x in range(plan.planes):
            first = x * grid + j * chunks
            turned[first : first + chunks, :] = total[x * chunks : (x + 1) * chunks]
    for r in range(turned.shape[0] // LANE):
        for c in range(turned.shape[1] // LANE):
            block = turned[r * LANE : (r + 1) * LANE, c * LANE : (c + 1) * LANE]
            out_ref[c * LANE : (c + 1) * LANE, r * LANE : (r + 1) * LANE] = block.T


def plane_work(plan, spread_ref, kernel_ref, yf_ref, yi_ref, xf_ref, xi_ref, out_ref, *lines):
    slabs, freqs, fold, wide = plan.slabs, plan.freqs, plan.fold, plan.wide
    padded, spectrum = plan.padded, plan.spectrum
    tiles = len(lines)
    for x in range(plan.planes):
        g, j = divmod(x, fold)
        start = g * plan.group + plan.starts[j]
        piece = split(spread_ref[:, start : start + wide])
        both = right_mul(piece, yf_ref[0, j], yf_ref[1, j])
        both = both.reshape(slabs, 2, freqs, 2 * padded)
        real = both[:, 0, :, :padded] + both[:, 1, :, padded:]
        imag = both[:, 1, :, :padded] - both[:, 0, :, padded:]
        mixed = jnp.stack([real, imag], axis=1).reshape(spectrum, padded)
        for t in range(tiles):
            lines[t][x * spectrum : (x + 1) * spectrum, :] = mixed[:, t * LANE : (t + 1) * LANE]

    def one_plane(k, carry):
        rows = pl.ds(k, plan.planes * slabs * 2, stride=freqs)
        field = jnp.concatenate([lines[t][rows, :] for t in range(tiles)], axis=1)
        spectra = left_mul(xf_ref[0], xf_ref[1], split(field))
        kernel = kernel_ref[k]
        spectra = jnp.concatenate(
            [spectra[: plan.period] * kernel, spectra[plan.period :] * kernel], axis=0
        )
        back = left_mul(xi_ref[0], xi_ref[1], split(spectra))
        for t in range(tiles):
            lines[t][rows, :] = back[:, t * LANE : (t + 1) * LANE]
        return carry

    lax.fori_loop(0, freqs, one_plane, 0)

    for g in range(plan.groups):
        total = [None] * (plan.group // LANE)
        for j in range(fold):
            x = g * fold + j
            if x >= plan.planes:
                break
            rows = slice(x * spectrum, (x + 1) * spectrum)
            field = jnp.concatenate([lines[t][rows, :] for t in range(tiles)], axis=1)
            both = right_mul(split(field), yi_ref[0, j], yi_ref[1, j])
            both = both.reshape(slabs, 2, freqs, 2 * wide)
            real = both[:, 0, :, :wide] - both[:, 1, :, wide:]
            imag = both[:, 1, :, :wide] + both[:, 0, :, wide:]
            mixed = jnp.stack([real, imag], axis=1).reshape(spectrum, wide)
            for t in range(wide // LANE):
                spot = plan.starts[j] // LANE + t
                term = mixed[:, t * LANE : (t + 1) * LANE]
                total[spot] = term if total[spot] is None else total[spot] + term
        for t, term in enumerate(total):
            if term is None:
                term = jnp.zeros((spectrum, LANE), jnp.float32)
            first = g * plan.group + t * LANE
            out_ref[:, first : first + LANE] = term


def inverse_z(plan, spread_ref, left_ref, right_ref, table_ref, near_ref, far_ref, turned):
    chunks, grid, wide = plan.chunks, plan.grid, plan.wide
    for r in range(turned.shape[0] // LANE):
        for c in range(turned.shape[1] // LANE):
            block = spread_ref[c * LANE : (c + 1) * LANE, r * LANE : (r + 1) * LANE]
            turned[r * LANE : (r + 1) * LANE, c * LANE : (c + 1) * LANE] = block.T
    total = [[None] * (plan.group // LANE) for _ in range(2)]
    for j in range(plan.fold):
        firsts = [x * grid + j * chunks for x in range(plan.planes)]
        rows = jnp.concatenate([turned[f : f + chunks, :] for f in firsts], axis=0)
        both = right_mul(split(rows), table_ref[0, j], table_ref[1, j])
        for i in range(2):
            for t in range(wide // LANE):
                spot = plan.starts[j] // LANE + t
                first = i * wide + t * LANE
                term = both[:, first : first + LANE]
                known = total[i][spot]
                total[i][spot] = term if known is None else known + term
    right = right_ref[...]
    far = None
    for i in range(2):
        field = jnp.concatenate(total[i], axis=1)
        near_ref[i] = field * right
        term = field * left_ref[i]
        far = term if far is None else far + term
    far_ref[...] = far


def call(body, outs, scratch, *operands):
    return pl.pallas_call(
        body,
        out_shape=outs,
        in_specs=[pl.BlockSpec(memory_space=pltpu.VMEM)] * len(operands),
        out_specs=jax.tree.map(lambda _: pl.BlockSpec(memory_space=pltpu.VMEM), outs),
        scratch_shapes=scratch,
        compiler_params=pltpu.CompilerParams(vmem_limit_bytes=60 * 2**20),
    )(*operands)


def is_wide(group, mask):
    lower = jnp.minimum(group, group ^ mask)
    return (group == lower) == (lower % 2 == 0)


def local(orbitals, occupation, kernel_hat, pair_mask):
    orbit_count, planes, plane_cells = orbitals.shape
    assert orbit_count == 2
    slabs = lax.axis_size("slab")
    groups = lax.axis_size("grp")
    plan = Plan(planes, plane_cells, slabs, kernel_hat.shape[0])
    tables = {name: jnp.asarray(t) for name, t in plan.tables().items()}
    f32 = jnp.float32
    flat = jax.ShapeDtypeStruct((plan.rows, plan.group), f32)
    twin = jax.ShapeDtypeStruct((2, plan.rows, plan.group), f32)
    spread = jax.ShapeDtypeStruct((plan.spectrum, plan.lanes), f32)
    turned = pltpu.VMEM((plan.lanes, plan.spectrum), f32)

    own_group = lax.axis_index("grp")
    partner_bits = pair_mask[0]
    wide_side = is_wide(own_group, partner_bits)
    scale = jnp.sqrt(0.25 * occupation.astype(f32))[:, None, None]
    own = (orbitals * scale).reshape(2, plan.rows, plan.group)

    def pairs(mask, wanted):
        chosen = []
        for g in range(groups):
            lower = min(g, g ^ mask)
            wide = (g == lower) == (lower % 2 == 0)
            if wanted is None or wide == wanted:
                chosen.append((g, g ^ mask))
        return chosen

    def exchange(mask):
        def run(own, kernel_hat):
            first = lax.ppermute(own[0], "grp", pairs(mask, None))
            second = lax.ppermute(own[1], "grp", pairs(mask, True))
            cube = kernel_hat.reshape(-1, plan.period, plan.period)
            cube = jnp.swapaxes(cube, 1, 2)
            cube = jnp.pad(cube, ((0, 0), (0, 0), (0, plan.padded - plan.period)))
            return first, second, cube

        return run

    def give_back(mask):
        def run(both, second):
            return (
                lax.ppermute(both, "grp", pairs(mask, None)),
                lax.ppermute(second, "grp", pairs(mask, False)),
            )

        return run

    masks = range(1, groups)
    index = partner_bits - 1
    first, second, cube = lax.switch(index, [exchange(m) for m in masks], own, kernel_hat)
    left = jnp.where(wide_side, own, jnp.stack([first, second]))
    right = jnp.where(wide_side, first, own[1])
    sent = call(
        lambda *refs: forward_z(plan, *refs), spread, [turned], left, right, tables["zf"]
    )
    here = lax.all_to_all(sent, "slab", split_axis=0, concat_axis=0, tiled=True)
    lines = [
        pltpu.VMEM((planes * plan.spectrum, LANE), f32) for _ in range(plan.padded // LANE)
    ]
    done = call(
        lambda *refs: plane_work(plan, *refs),
        spread,
        lines,
        here,
        cube,
        tables["yf"],
        tables["yi"],
        tables["xf"],
        tables["xi"],
    )
    back = lax.all_to_all(done, "slab", split_axis=0, concat_axis=0, tiled=True)
    near, far = call(
        lambda *refs: inverse_z(plan, *refs),
        (twin, flat),
        [turned],
        back,
        left,
        right,
        tables["zi"],
    )
    back_first, back_second = lax.switch(
        index, [give_back(m) for m in masks], jnp.where(wide_side, far, near[0]), near[1]
    )
    row_first = back_first + jnp.where(wide_side, near[0], 0.0)
    row_second = jnp.where(wide_side, near[1] + back_second, far)
    total = jnp.stack([row_first, row_second]).reshape(orbitals.shape)
    return total * (-1.0 / scale)


def solution(mesh):
    return jax.shard_map(
        local,
        mesh=mesh,
        in_specs=(P("grp", "slab", None), P("grp"), P("slab", None), P()),
        out_specs=P("grp", "slab", None),
        check_vma=False,
    )
```

```python
import math

import jax
import jax.numpy as jnp
import ml_dtypes
import numpy as np
from jax import lax
from jax.experimental import pallas as pl
from jax.experimental.pallas import tpu as pltpu
from jax.sharding import PartitionSpec as P

LANE = 128


def halves(table):
    high = table.astype(np.float32).astype(ml_dtypes.bfloat16)
    low = (table - high.astype(np.float64)).astype(ml_dtypes.bfloat16)
    return np.stack([high, low])


class Plan:
    def __init__(self, planes, plane_cells, slabs, freqs):
        self.planes = planes
        self.grid = math.isqrt(plane_cells)
        self.slabs = slabs
        self.freqs = freqs
        self.period = 2 * self.grid
        self.group = math.lcm(self.grid, LANE)
        self.fold = self.group // self.grid
        self.chunks = self.grid // self.fold
        self.rows = planes * self.chunks
        self.groups = -(-planes // self.fold)
        self.lanes = self.groups * self.group
        self.wide = 2 * LANE
        self.starts = []
        for fold in range(self.fold):
            start = fold * self.grid // LANE * LANE
            self.starts.append(min(start, self.group - self.wide))
        self.spectrum = 2 * self.period
        self.sub = LANE // (2 * slabs)
        self.parts = freqs // self.sub
        self.block = 2 * self.sub
        self.padded = -(-self.period // self.wide) * self.wide

    def wave(self, left, right):
        angle = 2.0 * math.pi / self.period * (np.outer(left, right) % self.period)
        return np.cos(angle), np.sin(angle)

    def tables(self):
        grid, period, fold = self.grid, self.period, self.fold
        cells = np.arange(grid)
        waves = np.arange(period)
        cos, sin = self.wave(cells, waves)
        cosi, sini = cos.T / period, sin.T / period
        column = [
            (c, owner * self.freqs + part * self.sub + own)
            for part in range(self.parts)
            for owner in range(self.slabs)
            for c in range(2)
            for own in range(self.sub)
        ]
        side = np.array([c[0] for c in column])
        freq = np.array([c[1] for c in column])
        offsets = [j * grid - self.starts[j] for j in range(fold)]
        reach = max(offsets)
        self.slides = [reach - offset for offset in offsets]
        zf = np.zeros((2, reach + self.wide, self.spectrum))
        zi = np.zeros((fold, self.spectrum, 2, self.wide))
        yf = np.zeros((reach + self.wide, 2, self.padded))
        yi = np.zeros((fold, self.padded, 2, self.wide))
        y_order = np.array([fold * q + j for j in range(fold) for q in range(self.chunks)])
        at = slice(reach, reach + grid)
        zf[0, at] = np.where(side == 0, cos[:, freq], -sin[:, freq])
        zf[1, at] = np.where(side == 0, sin[:, freq], cos[:, freq])
        yf[at, 0, :period] = cos[y_order]
        yf[at, 1, :period] = sin[y_order]
        for j in range(fold):
            at = slice(j * grid - self.starts[j], (j + 1) * grid - self.starts[j])
            zi[j, :, 0, at] = np.where(side == 0, cosi[freq].T, -sini[freq].T).T
            zi[j, :, 1, at] = np.where(side == 0, sini[freq].T, cosi[freq].T).T
            yi[j, :period, 0, at] = cosi[:, y_order]
            yi[j, :period, 1, at] = sini[:, y_order]
        row = [
            (c, s * self.planes + x)
            for x in range(self.planes)
            for s in range(self.slabs)
            for c in range(2)
        ]
        side = np.array([r[0] for r in row])
        cell = np.array([r[1] for r in row])
        xf = np.concatenate(
            [
                np.where(side == 0, cos[cell].T, sin[cell].T),
                np.where(side == 0, -sin[cell].T, cos[cell].T),
            ]
        )
        xi = np.concatenate(
            [
                np.where(side == 0, cosi[:, cell], sini[:, cell]),
                np.where(side == 0, -sini[:, cell], cosi[:, cell]),
            ]
        ).T
        return {
            "zf": halves(zf),
            "zi": halves(zi.reshape(fold, self.spectrum, 2 * self.wide)),
            "yf": halves(yf.reshape(-1, 2 * self.padded)),
            "yi": halves(yi.reshape(fold, self.padded, 2 * self.wide)),
            "xf": halves(xf),
            "xi": halves(xi),
        }


def mm(left, right):
    return jnp.dot(left, right, preferred_element_type=jnp.float32)


def split(value):
    high = value.astype(jnp.bfloat16)
    low = (value - high.astype(jnp.float32)).astype(jnp.bfloat16)
    return high, low


def right_mul(value, high, low):
    vh, vl = value
    return mm(vh, high) + mm(vh, low) + mm(vl, high)


def left_mul(high, low, value):
    vh, vl = value
    return mm(high, vh) + mm(low, vh) + mm(high, vl)


def forward_z(plan, left, right, table_ref, turned):
    densities = [split(field * right) for field in left]
    chunks, grid, wide = plan.chunks, plan.grid, plan.wide
    used = plan.planes * grid
    if used < plan.lanes:
        turned[used:, :] = jnp.zeros((plan.lanes - used, plan.spectrum), jnp.float32)
    for j in range(plan.fold):
        at = slice(plan.starts[j], plan.starts[j] + wide)
        rows = slice(plan.slides[j], plan.slides[j] + wide)
        total = None
        for i in range(2):
            piece = tuple(d[:, at] for d in densities[i])
            term = right_mul(piece, table_ref[0, i, rows], table_ref[1, i, rows])
            total = term if total is None else total + term
        for x in range(plan.planes):
            first = x * grid + j * chunks
            turned[first : first + chunks, :] = total[x * chunks : (x + 1) * chunks]


def turn_out(plan, part, turned, out_ref):
    size = plan.slabs * plan.block
    for c in range(0, size, LANE):
        for r in range(0, plan.lanes, LANE):
            block = turned[r : r + LANE, part * size + c : part * size + c + LANE].T
            out_ref[part, c // plan.block : (c + LANE) // plan.block, :, r : r + LANE] = (
                block.reshape(LANE // plan.block, plan.block, LANE)
            )


def plane_work(plan, part, spread_ref, kernel_ref, yf_ref, yi_ref, xf_ref, xi_ref, out_ref, lines):
    slabs, sub, fold, wide = plan.slabs, plan.sub, plan.fold, plan.wide
    padded, size = plan.padded, plan.slabs * plan.block
    tiles = len(lines)
    for x in range(plan.planes):
        g, j = divmod(x, fold)
        start = g * plan.group + plan.starts[j]
        piece = split(spread_ref[part, :, :, start : start + wide].reshape(size, wide))
        rows = slice(plan.slides[j], plan.slides[j] + wide)
        both = right_mul(piece, yf_ref[0, rows], yf_ref[1, rows])
        both = both.reshape(slabs, 2, sub, 2 * padded)
        real = both[:, 0, :, :padded] + both[:, 1, :, padded:]
        imag = both[:, 1, :, :padded] - both[:, 0, :, padded:]
        mixed = jnp.stack([real, imag], axis=1).reshape(size, padded)
        for t in range(tiles):
            lines[t][x * size : (x + 1) * size, :] = mixed[:, t * LANE : (t + 1) * LANE]

    def one_plane(k, carry):
        rows = pl.ds(k, plan.planes * slabs * 2, stride=sub)
        field = jnp.concatenate([lines[t][rows, :] for t in range(tiles)], axis=1)
        spectra = left_mul(xf_ref[0], xf_ref[1], split(field))
        kernel = kernel_ref[part * sub + k]
        spectra = jnp.concatenate(
            [spectra[: plan.period] * kernel, spectra[plan.period :] * kernel], axis=0
        )
        back = left_mul(xi_ref[0], xi_ref[1], split(spectra))
        for t in range(tiles):
            lines[t][rows, :] = back[:, t * LANE : (t + 1) * LANE]
        return carry

    lax.fori_loop(0, sub, one_plane, 0)

    for g in range(plan.groups):
        total = [None] * (plan.group // LANE)
        for j in range(fold):
            x = g * fold + j
            if x >= plan.planes:
                break
            rows = slice(x * size, (x + 1) * size)
            field = jnp.concatenate([lines[t][rows, :] for t in range(tiles)], axis=1)
            both = right_mul(split(field), yi_ref[0, j], yi_ref[1, j])
            both = both.reshape(slabs, 2, sub, 2 * wide)
            real = both[:, 0, :, :wide] - both[:, 1, :, wide:]
            imag = both[:, 1, :, :wide] + both[:, 0, :, wide:]
            mixed = jnp.stack([real, imag], axis=1).reshape(size, wide)
            for t in range(wide // LANE):
                spot = plan.starts[j] // LANE + t
                term = mixed[:, t * LANE : (t + 1) * LANE]
                total[spot] = term if total[spot] is None else total[spot] + term
        for t, term in enumerate(total):
            if term is None:
                term = jnp.zeros((size, LANE), jnp.float32)
            first = g * plan.group + t * LANE
            out_ref[part, :, :, first : first + LANE] = term.reshape(slabs, plan.block, LANE)


def inverse_z(plan, part, spread_ref, table_ref, turned, field_ref):
    chunks, grid, wide = plan.chunks, plan.grid, plan.wide
    size = plan.slabs * plan.block
    for r in range(0, plan.lanes, LANE):
        for c in range(0, size, LANE):
            block = spread_ref[part, c // plan.block : (c + LANE) // plan.block, :, r : r + LANE]
            turned[r : r + LANE, c : c + LANE] = block.reshape(LANE, LANE).T
    total = [[None] * (plan.group // LANE) for _ in range(2)]
    own = slice(part * size, (part + 1) * size)
    for j in range(plan.fold):
        firsts = [x * grid + j * chunks for x in range(plan.planes)]
        rows = jnp.concatenate([turned[f : f + chunks, :size] for f in firsts], axis=0)
        both = right_mul(split(rows), table_ref[0, j, own], table_ref[1, j, own])
        for i in range(2):
            for t in range(wide // LANE):
                spot = plan.starts[j] // LANE + t
                first = i * wide + t * LANE
                term = both[:, first : first + LANE]
                known = total[i][spot]
                total[i][spot] = term if known is None else known + term
    for i in range(2):
        field = jnp.concatenate(total[i], axis=1)
        field_ref[i] = field if part == 0 else field_ref[i] + field


NAMES = ("zf", "yf", "xf", "cube", "xi", "yi", "zi")


def core(plan, *refs):
    flag_ref, *hbm = refs[:12]
    sent_ref, kept_ref = refs[12:14]
    vmem = refs[14:25]
    turned, going, coming, leaving, landing, field = refs[25:31]
    load_sem, send_sem, recv_sem = refs[31:34]
    lines = refs[34:]
    slabs, parts = plan.slabs, plan.parts
    loads = [
        pltpu.make_async_copy(source, dest, load_sem.at[n])
        for n, (source, dest) in enumerate(zip(hbm, vmem))
    ]
    for load in loads:
        load.start()
    me = lax.axis_index("slab")
    steps = sorted(range(1, slabs), key=lambda step: -step)
    barrier = pltpu.get_barrier_semaphore()
    for step in steps:
        pl.semaphore_signal(
            barrier, 1, device_id={"slab": me ^ step}, device_id_type=pl.DeviceIdType.MESH
        )
    pl.semaphore_wait(barrier, slabs - 1)

    def own_copy(way, part):
        source, dest = ((going, coming), (leaving, landing))[way]
        return pltpu.make_async_copy(
            source.at[part, me], dest.at[part, me], recv_sem.at[way, part, 0]
        )

    def remote(way, part, step, arriving):
        source, dest = ((going, coming), (leaving, landing))[way]
        peer = me ^ step
        return pltpu.make_async_remote_copy(
            src_ref=source.at[part, peer],
            dst_ref=dest.at[part, peer if arriving else me],
            send_sem=send_sem.at[way, part, step],
            recv_sem=recv_sem.at[way, part, step],
            device_id={"slab": peer},
            device_id_type=pl.DeviceIdType.MESH,
        )

    def send(way, part):
        for step in steps:
            remote(way, part, step, False).start()
        own_copy(way, part).start()

    def receive(way, part):
        own_copy(way, part).wait()
        for step in steps:
            remote(way, part, step, True).wait_recv()

    for load in loads[:5]:
        load.wait()
    own_first, own_second, first, second, zf, yf, xf, cube, xi, yi, zi = vmem
    flag = flag_ref[0] > 0
    left = [
        jnp.where(flag, own_first[...], first[...]),
        jnp.where(flag, own_second[...], second[...]),
    ]
    right = jnp.where(flag, first[...], own_second[...])
    forward_z(plan, left, right, zf, turned)
    for part in range(parts):
        turn_out(plan, part, turned, going)
        send(0, part)
    for load in loads[5:]:
        load.wait()
    for part in range(parts):
        receive(0, part)
        plane_work(plan, part, coming, cube, yf, yi, xf, xi, leaving, lines)
        send(1, part)
    for part in range(parts):
        receive(1, part)
        inverse_z(plan, part, landing, zi, turned, field)
    near = [field[0] * right, field[1] * right]
    far = field[0] * left[0] + field[1] * left[1]
    sent_ref[0] = jnp.where(flag, far, near[0])
    sent_ref[1] = near[1]
    kept_ref[0] = jnp.where(flag, near[0], jnp.zeros_like(far))
    kept_ref[1] = jnp.where(flag, near[1], far)
    for way in range(2):
        for part in range(parts):
            for step in steps:
                remote(way, part, step, False).wait_send()


def run_core(plan, flag, fields, tables, cube):
    f32 = jnp.float32
    operands = list(fields) + [cube if name == "cube" else tables[name] for name in NAMES]
    twin = jax.ShapeDtypeStruct((2, plan.rows, plan.group), f32)
    blocks = pltpu.VMEM((plan.parts, plan.slabs, plan.block, plan.lanes), f32)
    line = pltpu.VMEM((plan.planes * plan.slabs * plan.block, LANE), f32)
    return pl.pallas_call(
        lambda *refs: core(plan, *refs),
        out_shape=(twin, twin),
        in_specs=[pl.BlockSpec(memory_space=pltpu.SMEM)]
        + [pl.BlockSpec(memory_space=pl.ANY)] * len(operands),
        out_specs=(pl.BlockSpec(memory_space=pltpu.VMEM),) * 2,
        scratch_shapes=[pltpu.VMEM(op.shape, op.dtype) for op in operands]
        + [pltpu.VMEM((plan.lanes, plan.spectrum), f32)]
        + [blocks] * 4
        + [
            pltpu.VMEM(twin.shape, f32),
            pltpu.SemaphoreType.DMA((len(operands),)),
            pltpu.SemaphoreType.DMA((2, plan.parts, plan.slabs)),
            pltpu.SemaphoreType.DMA((2, plan.parts, plan.slabs)),
        ]
        + [line] * (plan.padded // LANE),
        compiler_params=pltpu.CompilerParams(
            collective_id=0, has_side_effects=True, vmem_limit_bytes=60 * 2**20
        ),
    )(flag, *operands)


def is_wide(group, mask):
    lower = jnp.minimum(group, group ^ mask)
    return (group == lower) == (lower % 2 == 0)


def local(orbitals, occupation, kernel_hat, pair_mask):
    orbit_count, planes, plane_cells = orbitals.shape
    assert orbit_count == 2
    slabs = lax.axis_size("slab")
    groups = lax.axis_size("grp")
    plan = Plan(planes, plane_cells, slabs, kernel_hat.shape[0])
    tables = {name: jnp.asarray(t) for name, t in plan.tables().items()}
    f32 = jnp.float32
    own_group = lax.axis_index("grp")
    partner_bits = pair_mask[0]
    wide_side = is_wide(own_group, partner_bits)
    scale = jnp.sqrt(0.25 * occupation.astype(f32))[:, None, None]
    own = [(orbitals[i] * scale[i]).reshape(plan.rows, plan.group) for i in range(2)]

    def pairs(mask, wanted):
        chosen = []
        for g in range(groups):
            lower = min(g, g ^ mask)
            wide = (g == lower) == (lower % 2 == 0)
            if wanted is None or wide == wanted:
                chosen.append((g, g ^ mask))
        return chosen

    def exchange(mask):
        def run(own, kernel_hat):
            first = lax.ppermute(own[0], "grp", pairs(mask, None))
            second = lax.ppermute(own[1], "grp", pairs(mask, True))
            cube = kernel_hat.reshape(-1, plan.period, plan.period)
            cube = jnp.swapaxes(cube, 1, 2)
            cube = jnp.pad(cube, ((0, 0), (0, 0), (0, plan.padded - plan.period)))
            return first, second, cube

        return run

    def give_back(mask):
        def run(sent):
            return (
                lax.ppermute(sent[0], "grp", pairs(mask, None)),
                lax.ppermute(sent[1], "grp", pairs(mask, False)),
            )

        return run

    masks = range(1, groups)
    index = partner_bits - 1
    first, second, cube = lax.switch(index, [exchange(m) for m in masks], own, kernel_hat)
    flag = wide_side.astype(jnp.int32).reshape(1)
    sent, kept = run_core(plan, flag, (own[0], own[1], first, second), tables, cube)
    back = lax.switch(index, [give_back(m) for m in masks], sent)
    total = [
        (kept[i] + back[i]).reshape(planes, plane_cells) * (-1.0 / scale[i]) for i in range(2)
    ]
    return jnp.stack(total)


def solution(mesh):
    return jax.shard_map(
        local,
        mesh=mesh,
        in_specs=(P("grp", "slab", None), P("grp"), P("slab", None), P()),
        out_specs=P("grp", "slab", None),
        check_vma=False,
    )
```
